32 devices in a mesh: seq: 16 (over z, y, x), head: 2 (over core).
Axes of the slice: x: 2, y: 2, z: 4, core: 2. Of those that a mesh axis runs over, the one named last changes fastest.
Arguments:
- queries: bfloat16 [3072, 4096], P('seq', 'head'), may hold values from -6 to 6
- key_states: bfloat16 [3072, 512], P('seq', 'head'), may hold values from -6 to 6
- value_states: bfloat16 [3072, 512], P('seq', 'head'), may hold values from -6 to 6
- positions: int32 [3072], P('seq'), may hold values from 0 to 3071, as said below
- out_weight: bfloat16 [4096, 4096], P('head'), may hold values from -0.125 to 0.125
Outputs:
- mixed: bfloat16 [3072, 4096], P('seq', 'head')
The draws below stay inside these ranges and needn't reach their ends.
Inputs may be any that keep to these rules, and one draw needn't show every extreme that they name: The sequence is cut into 32 blocks of 96 consecutive positions. The 192 rows of one index of seq hold two whole blocks in order, block b and block 31 - b for some b below 16, each block's positions ascending; every position appears once.
All inputs are finite; a program needn't handle non-finite values.
Results may differ from the reference program's by a relative error of at most 0.0095.
Values may be sent and summed in bfloat16 or wider, within the bound.
A program may use at most 128 MiB of HBM per device.

```python
import jax
import jax.numpy as jnp
from jax import lax

HQ = 32
KV = 4
HD = 128
DOUT = 4096
GROUP = 8
TOK_DEV = 192
BLK = 96
BLOCKS = 32
TOKENS = 3072
N_SEQ = 16


def layout(key):
    order = jax.random.permutation(jax.random.fold_in(key, 101), N_SEQ).astype(jnp.int32)
    rows_all = jnp.arange(TOKENS, dtype=jnp.int32)
    device = rows_all // TOK_DEV
    within = rows_all % TOK_DEV
    second = within // BLK
    offset = within % BLK
    first_block = order[device]
    chosen_block = jnp.where(second == 1, BLOCKS - 1 - first_block, first_block)
    return (chosen_block * BLK + offset).astype(jnp.int32)


def draw_queries(key, part):
    places = layout(key)
    base = jnp.clip(4.0 * jax.random.normal(jax.random.fold_in(key, 1), (TOKENS, KV, GROUP, HD), jnp.float32), -6.0, 6.0)
    return base.reshape(TOKENS, HQ * HD)[places].astype(jnp.bfloat16)


def draw_key_states(key, part):
    places = layout(key)
    base = jnp.clip(jax.random.normal(jax.random.fold_in(key, 2), (TOKENS, KV, HD), jnp.float32), -6.0, 6.0)
    return base.reshape(TOKENS, KV * HD)[places].astype(jnp.bfloat16)


def draw_positions(key, part):
    return layout(key)


def strengthened(entries, stream_key, source, target, parts, factor):
    owner, partner = [(jnp.arange(entries.shape[position]) // (entries.shape[position] // parts)).reshape([-1 if axis == position else 1 for axis in range(entries.ndim)]) for position in (source, target)]
    chosen = jax.random.permutation(stream_key, parts)[partner]
    strong = (owner == chosen) | (owner == (partner + parts // 2) % parts)
    return jnp.where(strong, factor * entries, entries)


def level_of(stream_key, extent, shards, least, largest):
    gain, own = 1.0, jax.random.fold_in(stream_key, 6)
    for position, shards_of in shards:
        steps = jnp.exp(jax.random.uniform(jax.random.fold_in(own, position), (shards_of,), jnp.float32, least / len(shards), largest / len(shards)))
        gain = gain * jnp.repeat(steps, extent[position] // shards_of).reshape([-1 if axis == position else 1 for axis in range(len(extent))])
    return gain


def bell_draw(key, shape, width, reach, split=(), kind=jnp.bfloat16):
    result = jax.random.normal(key, shape, jnp.float32) * width
    if len(split) > 0:
        result = level_of(key, shape, split, -0.22, 0.18) * result
    return jnp.clip(result, min=-reach, max=reach).astype(kind)


def noise_with(key, shape, deviation, most, shards, heavy, held_as=jnp.bfloat16):
    values = deviation * jax.random.normal(key, shape, jnp.float32)
    if shards:
        values = values * level_of(key, shape, shards, -0.22, 0.18)
    return jnp.clip(strengthened(values, jax.random.fold_in(key, 3), *heavy), -most, most).astype(held_as)


def setup_inputs(seed: int = 0) -> dict:
    key_list = jax.random.split(jax.random.key(seed), 6)
    queries = draw_queries(jax.random.fold_in(key_list[5], 71), 0)
    key_states = draw_key_states(jax.random.fold_in(key_list[5], 71), 0)
    value_states = bell_draw(key_list[2], (TOKENS, KV * HD), 1.0, 6.0, ((0, 16), (1, 2)))
    positions = draw_positions(jax.random.fold_in(key_list[5], 71), 0)
    out_weight = noise_with(key_list[4], (HQ * HD, DOUT), (HQ * HD) ** -0.5, 0.125, ((0, 2),), (0, 1, 2, 2.0))
    return {"queries": queries, "key_states": key_states, "value_states": value_states, "positions": positions, "out_weight": out_weight}


def reference(queries, key_states, value_states, positions, out_weight):
    score_scale = HD ** -0.5
    query_all = queries.astype(jnp.float32).reshape(TOKENS // TOK_DEV, TOK_DEV, KV, GROUP, HD)
    key_heads = key_states.astype(jnp.float32).reshape(TOKENS, KV, HD).transpose(1, 0, 2)
    value_heads = value_states.astype(jnp.float32).reshape(TOKENS, KV, HD).transpose(1, 0, 2)
    place_blocks = positions.reshape(TOKENS // TOK_DEV, TOK_DEV)

    def per_block(query_pair):
        query_block, query_place = query_pair
        visible = positions[None, None, :] <= query_place[None, :, None]

        def per_head(head_items):
            query_head, key_head, value_head = head_items
            scores = jnp.einsum("tgd,kd->gtk", query_head, key_head) * score_scale
            row_peak = jnp.max(jnp.where(visible, scores, -jnp.inf), axis=-1, keepdims=True)
            weights = jnp.where(visible, jnp.exp(scores - row_peak), 0.0)
            row_total = jnp.sum(weights, axis=-1, keepdims=True)
            rounded = lax.optimization_barrier(weights.astype(jnp.bfloat16)).astype(jnp.float32)
            return jnp.einsum("gtk,kd->gtd", rounded, value_head) / row_total

        heads_out = lax.map(per_head, (query_block.transpose(1, 0, 2, 3), key_heads, value_heads))
        return heads_out.transpose(2, 0, 1, 3).reshape(TOK_DEV, HQ * HD).astype(jnp.bfloat16)

    attended = lax.map(per_block, (query_all, place_blocks)).reshape(TOKENS, HQ * HD)
    return jnp.dot(attended, out_weight, preferred_element_type=jnp.float32).astype(jnp.bfloat16)
```

```python
import functools

import jax
import jax.numpy as jnp
from jax import lax
from jax.experimental import pallas as pl
from jax.experimental.pallas import tpu as pltpu
from jax.sharding import PartitionSpec as P

HD = 128
GROUP = 8
MESH = pl.DeviceIdType.MESH
LOG2E = 1.4426950408889634
FAR = 1e30

ORDERS = ("zxy", "yzx", "zyx", "xzy")


def kernel(
    n, heads, lanes, q_ref, k_ref, v_ref, place_ref, mark_ref, w_hbm, out_ref,
    kv, marks, q_t, acc, top, total, att, w, part, sent, got,
    send_sem, recv_sem, mark_send, mark_recv, w_sem, out_send, out_recv,
):
    rows = q_ref.shape[0]
    half = rows // 2
    groups = k_ref.shape[1] // HD
    width = GROUP * rows
    streams = 2 * groups
    depth = n // 4
    scale = HD ** -0.5 * LOG2E

    me = lax.axis_index("seq")
    head = lax.axis_index("head")
    z = me // 4
    y = lax.rem(me // 2, 2)
    x = lax.rem(me, 2)
    along_x = me + 1 - 2 * x
    along_y = me + 2 - 4 * y
    above = me + 4
    below = me - 4
    has_above = z < depth - 1
    has_below = z > 0

    load_w = pltpu.make_async_copy(w_hbm, w, w_sem)
    load_w.start()

    barrier = pltpu.get_barrier_semaphore()

    def greet(seq_index, head_index):
        pl.semaphore_signal(barrier, inc=1, device_id=(seq_index, head_index), device_id_type=MESH)

    greet(along_x, head)
    greet(along_y, head)
    for step in range(1, heads):
        greet(me, lax.rem(head + step, heads))

    @pl.when(has_above)
    def _():
        greet(above, head)

    @pl.when(has_below)
    def _():
        greet(below, head)

    peers = 1 + heads + has_above.astype(jnp.int32) + has_below.astype(jnp.int32)
    pl.semaphore_wait(barrier, peers)

    def routes(source, order):
        s_z = source // 4
        same = {"y": lax.rem(source // 2, 2) == y, "x": lax.rem(source, 2) == x, "z": s_z == z}
        found = []
        for spot, axis in enumerate(order):
            later = [same[other] for other in order[spot + 1:]]
            if axis == "z":
                ways = [([z >= s_z, has_above], above, 0), ([z <= s_z, has_below], below, 1)]
            elif axis == "x":
                ways = [([same["x"]], along_x, 2)]
            else:
                ways = [([same["y"]], along_y, 3)]
            for terms, target, way in ways:
                condition = functools.reduce(jnp.logical_and, terms + later)
                found.append((condition, target, way))
        return found

    def each_copy(source, stream, own, act):
        if stream == streams:
            order = ORDERS[0]
            src = mark_ref if own else marks.at[source]
            dst = marks.at[source]
            sems = lambda way: (mark_send.at[source, way], mark_recv.at[source])
        else:
            order = ORDERS[stream % len(ORDERS)]
            given = (k_ref, v_ref)[stream % 2]
            g = stream // 2
            src = given.at[:, g * HD:(g + 1) * HD] if own else kv.at[source, stream]
            dst = kv.at[source, stream]
            sems = lambda way: (send_sem.at[source, stream, way], recv_sem.at[source, stream])
        for condition, target, way in routes(source, order):
            out_sem, in_sem = sems(way)
            copy = pltpu.make_async_remote_copy(
                src_ref=src, dst_ref=dst, send_sem=out_sem, recv_sem=in_sem,
                device_id=(target, head), device_id_type=MESH,
            )

            @pl.when(condition)
            def _(copy=copy):
                act(copy)

    def arrive(source, stream):
        if stream == streams:
            dst, out_sem, in_sem = marks.at[source], mark_send.at[source, 0], mark_recv.at[source]
        else:
            dst = kv.at[source, stream]
            out_sem, in_sem = send_sem.at[source, stream, 0], recv_sem.at[source, stream]
        pltpu.make_async_remote_copy(
            src_ref=dst, dst_ref=dst, send_sem=out_sem, recv_sem=in_sem,
            device_id=(along_x, head), device_id_type=MESH,
        ).wait_recv()
        each_copy(source, stream, False, lambda copy: copy.start())

    def source_of(turn):
        k = turn // 4
        rest = lax.rem(turn, 4)
        edge = jnp.minimum(z, depth - 1 - z)
        near = z + jnp.where(lax.rem(k, 2) == 1, -((k + 1) // 2), k // 2)
        wide = jnp.where(2 * z < depth - 1, k, depth - 1 - k)
        s_z = jnp.where(k <= 2 * edge, near, wide)
        s_y = lax.rem(y + rest // 2, 2)
        s_x = lax.rem(x + lax.rem(rest, 2), 2)
        return s_z * 4 + s_y * 2 + s_x

    for stream in [streams] + list(range(streams)):
        each_copy(me, stream, True, lambda copy: copy.start())

    chunks = [slice(c, c + lanes) for c in range(0, width, lanes)]

    for g in range(groups):
        for h in range(GROUP):
            column = (g * GROUP + h) * HD
            att[h * rows:(h + 1) * rows, :] = q_ref[:, column:column + HD]
        q_t[g] = att[...].T

    for g in range(groups):
        key_rows = k_ref[:, g * HD:(g + 1) * HD]
        value_cols = v_ref[:, g * HD:(g + 1) * HD]
        for cols in chunks:
            scores = jnp.dot(key_rows, q_t[g, :, cols], preferred_element_type=jnp.float32)
            key_row = lax.broadcasted_iota(jnp.int32, (rows, lanes), 0)
            query_row = lax.rem(lax.broadcasted_iota(jnp.int32, (rows, lanes), 1) + cols.start, rows)
            seen = key_row <= query_row
            peak = jnp.max(jnp.where(seen, scores, -FAR), axis=0, keepdims=True)
            weights = jnp.where(seen, jnp.exp2((scores - peak) * scale), 0.0)
            top[g, :, cols] = peak
            total[g, :, cols] = jnp.sum(weights, axis=0, keepdims=True)
            acc[g, :, cols] = lax.dot_general(
                value_cols, weights.astype(jnp.bfloat16), (((0,), (0,)), ((), ())),
                preferred_element_type=jnp.float32,
            )

    def attend(source, g):
        key_rows = kv[source, 2 * g]
        value_cols = kv[source, 2 * g + 1]
        mark = marks[source]
        firsts = [jnp.concatenate([mark[b:b + 1, :]] * (lanes // HD), axis=1) for b in range(2)]
        for cols in chunks:
            scores = jnp.dot(key_rows, q_t[g, :, cols], preferred_element_type=jnp.float32)
            place = place_ref[:, cols]
            old = top[g, :, cols]
            peak = old
            seen, blocks = [], []
            for b in range(2):
                block = scores[b * half:(b + 1) * half]
                visible = firsts[b] <= place
                peak = jnp.maximum(
                    peak, jnp.where(visible, jnp.max(block, axis=0, keepdims=True), -FAR)
                )
                seen.append(visible)
                blocks.append(block)
            shift = peak * scale
            factor = jnp.exp2((old - peak) * scale)
            weights = jnp.concatenate(
                [
                    jnp.exp2(blocks[b] * scale - jnp.where(seen[b], shift, FAR))
                    for b in range(2)
                ],
                axis=0,
            )
            top[g, :, cols] = peak
            total[g, :, cols] = total[g, :, cols] * factor + jnp.sum(weights, axis=0, keepdims=True)
            acc[g, :, cols] = acc[g, :, cols] * factor + lax.dot_general(
                value_cols, weights.astype(jnp.bfloat16), (((0,), (0,)), ((), ())),
                preferred_element_type=jnp.float32,
            )

    first = source_of(1)
    for stream in [streams] + list(range(streams)):
        arrive(first, stream)

    def turn_body(turn, carry):
        source = source_of(turn)
        ahead = source_of(turn + 1)
        arrive(ahead, streams)
        for g in range(groups):
            arrive(ahead, 2 * g)
            arrive(ahead, 2 * g + 1)
            attend(source, g)
        return carry

    lax.fori_loop(1, n - 1, turn_body, 0)
    last = source_of(n - 1)
    for g in range(groups):
        attend(last, g)

    load_w.wait()
    for g in range(groups):
        share = (acc[g] * (1.0 / total[g])).astype(jnp.bfloat16)
        att[...] = share.T
        for h in range(GROUP):
            column = (g * GROUP + h) * HD
            part[:, column:column + HD] = att[h * rows:(h + 1) * rows, :]

    out_cols = out_ref.shape[1]
    tile = sent.shape[-1]
    tiles = out_cols // tile

    def product(owner, number):
        begin = pl.multiple_of(owner * out_cols + number * tile, tile)
        return jnp.dot(part[...], w[:, pl.ds(begin, tile)], preferred_element_type=jnp.float32)

    def out_copy(step, number):
        return pltpu.make_async_remote_copy(
            src_ref=sent.at[step - 1, number], dst_ref=got.at[step - 1, number],
            send_sem=out_send.at[step - 1, number], recv_sem=out_recv.at[step - 1, number],
            device_id=(me, lax.rem(head + step, heads)), device_id_type=MESH,
        )

    for step in range(1, heads):
        owner = lax.rem(head + step, heads)

        def send_tile(number, carry, step=step, owner=owner):
            sent[step - 1, number] = product(owner, number).astype(jnp.bfloat16)
            out_copy(step, number).start()
            return carry

        lax.fori_loop(0, tiles, send_tile, 0)

    def own_tile(number, carry):
        value = product(head, number)
        for step in range(1, heads):
            out_copy(step, number).wait_recv()
            value = value + got[step - 1, number].astype(jnp.float32)
        out_ref[:, pl.ds(pl.multiple_of(number * tile, tile), tile)] = value.astype(out_ref.dtype)
        return carry

    lax.fori_loop(0, tiles, own_tile, 0)

    def finish(number, carry):
        for step in range(1, heads):
            out_copy(step, number).wait_send()
        return carry

    lax.fori_loop(0, tiles, finish, 0)

    for stream in range(streams + 1):
        each_copy(me, stream, True, lambda copy: copy.wait_send())

    def close(turn, carry):
        source = source_of(turn)
        for stream in range(streams + 1):
            each_copy(source, stream, False, lambda copy: copy.wait_send())
        return carry

    lax.fori_loop(1, n, close, 0)


def shards(n, heads, queries, key_states, value_states, positions, out_weight):
    rows = queries.shape[0]
    half = rows // 2
    groups = key_states.shape[1] // HD
    streams = 2 * groups
    width = GROUP * rows
    out_cols = out_weight.shape[1] // heads
    tile = min(512, out_cols)
    tiles = out_cols // tile
    place = jnp.tile(positions, GROUP)[None]
    mark = jnp.broadcast_to(jnp.repeat(positions[::half], 4)[:, None], (8, HD))
    mark = jnp.concatenate([mark[0:1], mark[4:5]] * 4, axis=0)
    vmem = pl.BlockSpec(memory_space=pltpu.VMEM)
    bf16, f32 = jnp.bfloat16, jnp.float32
    dma = pltpu.SemaphoreType.DMA
    return pl.pallas_call(
        functools.partial(kernel, n, heads, 256),
        out_shape=jax.ShapeDtypeStruct((rows, out_cols), bf16),
        in_specs=[vmem] * 5 + [pl.BlockSpec(memory_space=pl.ANY)],
        out_specs=vmem,
        scratch_shapes=[
            pltpu.VMEM((n, streams, rows, HD), bf16),
            pltpu.VMEM((n, 8, HD), jnp.int32),
            pltpu.VMEM((groups, HD, width), bf16),
            pltpu.VMEM((groups, HD, width), f32),
            pltpu.VMEM((groups, 1, width), f32),
            pltpu.VMEM((groups, 1, width), f32),
            pltpu.VMEM((width, HD), bf16),
            pltpu.VMEM(out_weight.shape, bf16),
            pltpu.VMEM((rows, out_weight.shape[0]), bf16),
            pltpu.VMEM((heads - 1, tiles, rows, tile), bf16),
            pltpu.VMEM((heads - 1, tiles, rows, tile), bf16),
            dma((n, streams, 4)),
            dma((n, streams)),
            dma((n, 4)),
            dma((n,)),
            dma,
            dma((heads - 1, tiles)),
            dma((heads - 1, tiles)),
        ],
        compiler_params=pltpu.CompilerParams(
            collective_id=0, has_side_effects=True, vmem_limit_bytes=60000 * 1024
        ),
    )(queries, key_states, value_states, place, mark, out_weight)


def solution(mesh):
    in_specs = (P("seq", "head"), P("seq", "head"), P("seq", "head"), P("seq"), P("head", None))
    out_specs = P("seq", "head")
    body = functools.partial(shards, mesh.shape["seq"], mesh.shape["head"])
    return jax.shard_map(body, mesh=mesh, in_specs=in_specs, out_specs=out_specs, check_vma=False)
```

```python
import functools

import jax
import jax.numpy as jnp
from jax import lax
from jax.experimental import pallas as pl
from jax.experimental.pallas import tpu as pltpu
from jax.sharding import PartitionSpec as P

HD = 128
GROUP = 8
MESH = pl.DeviceIdType.MESH
LOG2E = 1.4426950408889634
FAR = 1e30

ORDERS = ("zxy", "yzx", "zyx", "xzy")


def kernel(
    n, heads, lanes, q_ref, k_ref, v_ref, first_ref, mark_ref, w_hbm, out_ref,
    kv, marks, place_row, q_t, acc, top, total, att, w, part, sent, got,
    send_sem, recv_sem, mark_send, mark_recv, w_sem, out_send, out_recv,
):
    rows = q_ref.shape[0]
    half = rows // 2
    groups = k_ref.shape[1] // HD
    width = GROUP * rows
    streams = 2 * groups
    depth = n // 4
    scale = HD ** -0.5 * LOG2E

    me = lax.axis_index("seq")
    head = lax.axis_index("head")
    z = me // 4
    y = lax.rem(me // 2, 2)
    x = lax.rem(me, 2)
    along_x = me + 1 - 2 * x
    along_y = me + 2 - 4 * y
    above = me + 4
    below = me - 4
    has_above = z < depth - 1
    has_below = z > 0

    load_w = pltpu.make_async_copy(w_hbm, w, w_sem)
    load_w.start()

    barrier = pltpu.get_barrier_semaphore()

    def greet(seq_index, head_index):
        pl.semaphore_signal(barrier, inc=1, device_id=(seq_index, head_index), device_id_type=MESH)

    greet(along_x, head)
    greet(along_y, head)
    for step in range(1, heads):
        greet(me, lax.rem(head + step, heads))

    @pl.when(has_above)
    def _():
        greet(above, head)

    @pl.when(has_below)
    def _():
        greet(below, head)

    peers = 1 + heads + has_above.astype(jnp.int32) + has_below.astype(jnp.int32)
    pl.semaphore_wait(barrier, peers)

    def routes(source, order):
        s_z = source // 4
        same = {"y": lax.rem(source // 2, 2) == y, "x": lax.rem(source, 2) == x, "z": s_z == z}
        found = []
        for spot, axis in enumerate(order):
            later = [same[other] for other in order[spot + 1:]]
            if axis == "z":
                ways = [([z >= s_z, has_above], above, 0), ([z <= s_z, has_below], below, 1)]
            elif axis == "x":
                ways = [([same["x"]], along_x, 2)]
            else:
                ways = [([same["y"]], along_y, 3)]
            for terms, target, way in ways:
                condition = functools.reduce(jnp.logical_and, terms + later)
                found.append((condition, target, way))
        return found

    def each_copy(source, stream, own, act):
        if stream == streams:
            order = ORDERS[0]
            src = mark_ref if own else marks.at[source]
            dst = marks.at[source]
            sems = lambda way: (mark_send.at[source, way], mark_recv.at[source])
        else:
            order = ORDERS[stream % len(ORDERS)]
            given = (k_ref, v_ref)[stream % 2]
            g = stream // 2
            src = given.at[:, g * HD:(g + 1) * HD] if own else kv.at[source, stream]
            dst = kv.at[source, stream]
            sems = lambda way: (send_sem.at[source, stream, way], recv_sem.at[source, stream])
        for condition, target, way in routes(source, order):
            out_sem, in_sem = sems(way)
            copy = pltpu.make_async_remote_copy(
                src_ref=src, dst_ref=dst, send_sem=out_sem, recv_sem=in_sem,
                device_id=(target, head), device_id_type=MESH,
            )

            @pl.when(condition)
            def _(copy=copy):
                act(copy)

    def arrive(source, stream):
        if stream == streams:
            dst, out_sem, in_sem = marks.at[source], mark_send.at[source, 0], mark_recv.at[source]
        else:
            dst = kv.at[source, stream]
            out_sem, in_sem = send_sem.at[source, stream, 0], recv_sem.at[source, stream]
        pltpu.make_async_remote_copy(
            src_ref=dst, dst_ref=dst, send_sem=out_sem, recv_sem=in_sem,
            device_id=(along_x, head), device_id_type=MESH,
        ).wait_recv()
        each_copy(source, stream, False, lambda copy: copy.start())

    wave = sorted(range(n), key=lambda c: (c // 4 + (c % 4 + 1) // 2, c))

    def source_of(turn):
        code = sum(jnp.where(turn == spot, value, 0) for spot, value in enumerate(wave))
        k = code // 4
        rest = lax.rem(code, 4)
        edge = jnp.minimum(z, depth - 1 - z)
        near = z + jnp.where(lax.rem(k, 2) == 1, -((k + 1) // 2), k // 2)
        wide = jnp.where(2 * z < depth - 1, k, depth - 1 - k)
        s_z = jnp.where(k <= 2 * edge, near, wide)
        s_y = lax.rem(y + rest // 2, 2)
        s_x = lax.rem(x + lax.rem(rest, 2), 2)
        return s_z * 4 + s_y * 2 + s_x

    for stream in [streams] + list(range(streams)):
        each_copy(me, stream, True, lambda copy: copy.start())

    chunks = [slice(c, c + lanes) for c in range(0, width, lanes)]

    for g in range(groups):
        for h in range(GROUP):
            column = (g * GROUP + h) * HD
            att[h * rows:(h + 1) * rows, :] = q_ref[:, column:column + HD]
        q_t[g] = att[...].T

    lane = lax.rem(lax.broadcasted_iota(jnp.int32, (1, width), 1), rows)
    place_row[...] = jnp.where(lane < half, first_ref[0], first_ref[half])

    for g in range(groups):
        key_rows = k_ref[:, g * HD:(g + 1) * HD]
        value_rows = v_ref[:, g * HD:(g + 1) * HD].T
        for cols in chunks:
            scores = jnp.dot(key_rows, q_t[g, :, cols], preferred_element_type=jnp.float32)
            key_row = lax.broadcasted_iota(jnp.int32, (rows, lanes), 0)
            query_row = lax.rem(lax.broadcasted_iota(jnp.int32, (1, lanes), 1) + cols.start, rows)
            seen = key_row <= query_row
            peak = jnp.max(jnp.where(seen, scores, -FAR), axis=0, keepdims=True)
            weights = jnp.where(seen, jnp.exp2((scores - peak) * scale), 0.0)
            top[g, :, cols] = peak
            total[g, :, cols] = jnp.sum(weights, axis=0, keepdims=True)
            acc[g, :, cols] = jnp.dot(
                value_rows, weights.astype(jnp.bfloat16), preferred_element_type=jnp.float32
            )

    def attend(source, g):
        key_rows = kv[source, 2 * g]
        value_rows = kv[source, 2 * g + 1].T
        mark = marks[source]
        firsts = [
            jnp.broadcast_to(mark[:, b * half:b * half + 1], (1, lanes)) for b in range(2)
        ]
        def score(number):
            return jnp.dot(key_rows, q_t[g, :, chunks[number]], preferred_element_type=jnp.float32)

        coming = score(0)
        for number, cols in enumerate(chunks):
            scores = coming
            if number + 1 < len(chunks):
                coming = score(number + 1)
            place = place_row[:, cols]
            old = top[g, :, cols]
            peak = old
            seen, blocks = [], []
            for b in range(2):
                block = scores[b * half:(b + 1) * half]
                visible = firsts[b] <= place
                peak = jnp.maximum(
                    peak, jnp.where(visible, jnp.max(block, axis=0, keepdims=True), -FAR)
                )
                seen.append(visible)
                blocks.append(block)
            shift = peak * scale
            factor = jnp.exp2((old - peak) * scale)
            weights = jnp.concatenate(
                [
                    jnp.exp2(blocks[b] * scale - jnp.where(seen[b], shift, FAR))
                    for b in range(2)
                ],
                axis=0,
            )
            top[g, :, cols] = peak
            total[g, :, cols] = total[g, :, cols] * factor + jnp.sum(weights, axis=0, keepdims=True)
            acc[g, :, cols] = acc[g, :, cols] * factor + jnp.dot(
                value_rows, weights.astype(jnp.bfloat16), preferred_element_type=jnp.float32
            )

    first = source_of(1)
    for stream in [streams] + list(range(streams)):
        arrive(first, stream)

    def turn_body(turn, carry):
        source = source_of(turn)
        ahead = source_of(turn + 1)
        arrive(ahead, streams)
        for g in range(groups):
            arrive(ahead, 2 * g)
            arrive(ahead, 2 * g + 1)
            attend(source, g)
        return carry

    lax.fori_loop(1, n - 1, turn_body, 0)
    last = source_of(n - 1)
    for g in range(groups):
        attend(last, g)

    load_w.wait()
    for g in range(groups):
        share = (acc[g] * (1.0 / total[g])).astype(jnp.bfloat16)
        att[...] = share.T
        for h in range(GROUP):
            column = (g * GROUP + h) * HD
            part[:, column:column + HD] = att[h * rows:(h + 1) * rows, :]

    out_cols = out_ref.shape[1]
    tile = sent.shape[-1]
    tiles = out_cols // tile

    def product(owner, number):
        begin = pl.multiple_of(owner * out_cols + number * tile, tile)
        return jnp.dot(part[...], w[:, pl.ds(begin, tile)], preferred_element_type=jnp.float32)

    def out_copy(step, number):
        return pltpu.make_async_remote_copy(
            src_ref=sent.at[step - 1, number], dst_ref=got.at[step - 1, number],
            send_sem=out_send.at[step - 1, number], recv_sem=out_recv.at[step - 1, number],
            device_id=(me, lax.rem(head + step, heads)), device_id_type=MESH,
        )

    for step in range(1, heads):
        owner = lax.rem(head + step, heads)

        def send_tile(number, carry, step=step, owner=owner):
            sent[step - 1, number] = product(owner, number).astype(jnp.bfloat16)
            out_copy(step, number).start()
            return carry

        lax.fori_loop(0, tiles, send_tile, 0)

    def own_tile(number, carry):
        value = product(head, number)
        for step in range(1, heads):
            out_copy(step, number).wait_recv()
            value = value + got[step - 1, number].astype(jnp.float32)
        out_ref[:, pl.ds(pl.multiple_of(number * tile, tile), tile)] = value.astype(out_ref.dtype)
        return carry

    lax.fori_loop(0, tiles, own_tile, 0)

    def finish(number, carry):
        for step in range(1, heads):
            out_copy(step, number).wait_send()
        return carry

    lax.fori_loop(0, tiles, finish, 0)

    for stream in range(streams + 1):
        each_copy(me, stream, True, lambda copy: copy.wait_send())

    def close(turn, carry):
        source = source_of(turn)
        for stream in range(streams + 1):
            each_copy(source, stream, False, lambda copy: copy.wait_send())
        return carry

    lax.fori_loop(1, n, close, 0)


def shards(n, heads, queries, key_states, value_states, positions, out_weight):
    rows = queries.shape[0]
    groups = key_states.shape[1] // HD
    streams = 2 * groups
    width = GROUP * rows
    out_cols = out_weight.shape[1] // heads
    tile = min(512, out_cols)
    tiles = out_cols // tile
    vmem = pl.BlockSpec(memory_space=pltpu.VMEM)
    bf16, f32 = jnp.bfloat16, jnp.float32
    dma = pltpu.SemaphoreType.DMA
    return pl.pallas_call(
        functools.partial(kernel, n, heads, 768),
        out_shape=jax.ShapeDtypeStruct((rows, out_cols), bf16),
        in_specs=[vmem] * 3 + [pl.BlockSpec(memory_space=pltpu.SMEM), vmem] + [pl.BlockSpec(memory_space=pl.ANY)],
        out_specs=vmem,
        scratch_shapes=[
            pltpu.VMEM((n, streams, rows, HD), bf16),
            pltpu.VMEM((n, 1, rows), jnp.int32),
            pltpu.VMEM((1, width), jnp.int32),
            pltpu.VMEM((groups, HD, width), bf16),
            pltpu.VMEM((groups, HD, width), f32),
            pltpu.VMEM((groups, 1, width), f32),
            pltpu.VMEM((groups, 1, width), f32),
            pltpu.VMEM((width, HD), bf16),
            pltpu.VMEM(out_weight.shape, bf16),
            pltpu.VMEM((rows, out_weight.shape[0]), bf16),
            pltpu.VMEM((heads - 1, tiles, rows, tile), bf16),
            pltpu.VMEM((heads - 1, tiles, rows, tile), bf16),
            dma((n, streams, 4)),
            dma((n, streams)),
            dma((n, 4)),
            dma((n,)),
            dma,
            dma((heads - 1, tiles)),
            dma((heads - 1, tiles)),
        ],
        compiler_params=pltpu.CompilerParams(
            collective_id=0, has_side_effects=True, vmem_limit_bytes=60000 * 1024
        ),
    )(queries, key_states, value_states, positions, positions[None], out_weight)


def solution(mesh):
    in_specs = (P("seq", "head"), P("seq", "head"), P("seq", "head"), P("seq"), P("head", None))
    out_specs = P("seq", "head")
    body = functools.partial(shards, mesh.shape["seq"], mesh.shape["head"])
    return jax.shard_map(body, mesh=mesh, in_specs=in_specs, out_specs=out_specs, check_vma=False)
```

```python
import functools

import jax
import jax.numpy as jnp
from jax import lax
from jax.experimental import pallas as pl
from jax.experimental.pallas import tpu as pltpu
from jax.sharding import PartitionSpec as P

HD = 128
GROUP = 8
MESH = pl.DeviceIdType.MESH
LOG2E = 1.4426950408889634
FAR = 1e30

ORDERS = ("zxy", "yzx", "zyx", "xzy")


def kernel(
    n, heads, lanes, q_ref, k_ref, v_ref, first_ref, mark_ref, w_hbm, out_ref,
    kv, marks, place_row, q_t, acc, top, total, att, w, part, sent, got,
    send_sem, recv_sem, mark_send, mark_recv, w_sem, out_send, out_recv,
):
    rows = q_ref.shape[0]
    half = rows // 2
    groups = k_ref.shape[1] // HD
    width = GROUP * rows
    streams = 2 * groups
    depth = n // 4
    scale = HD ** -0.5 * LOG2E

    me = lax.axis_index("seq")
    head = lax.axis_index("head")
    z = me // 4
    y = lax.rem(me // 2, 2)
    x = lax.rem(me, 2)
    along_x = me + 1 - 2 * x
    along_y = me + 2 - 4 * y
    above = me + 4
    below = me - 4
    has_above = z < depth - 1
    has_below = z > 0

    load_w = pltpu.make_async_copy(w_hbm, w, w_sem)
    load_w.start()

    barrier = pltpu.get_barrier_semaphore()

    def greet(seq_index, head_index):
        pl.semaphore_signal(barrier, inc=1, device_id=(seq_index, head_index), device_id_type=MESH)

    greet(along_x, head)
    greet(along_y, head)
    for step in range(1, heads):
        greet(me, lax.rem(head + step, heads))

    @pl.when(has_above)
    def _():
        greet(above, head)

    @pl.when(has_below)
    def _():
        greet(below, head)

    peers = 1 + heads + has_above.astype(jnp.int32) + has_below.astype(jnp.int32)
    pl.semaphore_wait(barrier, peers)

    def routes(source, order):
        s_z = source // 4
        same = {"y": lax.rem(source // 2, 2) == y, "x": lax.rem(source, 2) == x, "z": s_z == z}
        found = []
        for spot, axis in enumerate(order):
            later = [same[other] for other in order[spot + 1:]]
            if axis == "z":
                ways = [([z >= s_z, has_above], above, 0), ([z <= s_z, has_below], below, 1)]
            elif axis == "x":
                ways = [([same["x"]], along_x, 2)]
            else:
                ways = [([same["y"]], along_y, 3)]
            for terms, target, way in ways:
                condition = functools.reduce(jnp.logical_and, terms + later)
                found.append((condition, target, way))
        return found

    def each_copy(source, stream, own, act):
        if stream == streams:
            order = ORDERS[0]
            src = mark_ref if own else marks.at[source]
            dst = marks.at[source]
            sems = lambda way: (mark_send.at[source, way], mark_recv.at[source])
        else:
            order = ORDERS[stream % len(ORDERS)]
            given = (k_ref, v_ref)[stream % 2]
            g = stream // 2
            src = given.at[:, g * HD:(g + 1) * HD] if own else kv.at[source, stream]
            dst = kv.at[source, stream]
            sems = lambda way: (send_sem.at[source, stream, way], recv_sem.at[source, stream])
        for condition, target, way in routes(source, order):
            out_sem, in_sem = sems(way)
            copy = pltpu.make_async_remote_copy(
                src_ref=src, dst_ref=dst, send_sem=out_sem, recv_sem=in_sem,
                device_id=(target, head), device_id_type=MESH,
            )

            @pl.when(condition)
            def _(copy=copy):
                act(copy)

    def arrive(source, stream):
        if stream == streams:
            dst, out_sem, in_sem = marks.at[source], mark_send.at[source, 0], mark_recv.at[source]
        else:
            dst = kv.at[source, stream]
            out_sem, in_sem = send_sem.at[source, stream, 0], recv_sem.at[source, stream]
        pltpu.make_async_remote_copy(
            src_ref=dst, dst_ref=dst, send_sem=out_sem, recv_sem=in_sem,
            device_id=(along_x, head), device_id_type=MESH,
        ).wait_recv()
        each_copy(source, stream, False, lambda copy: copy.start())

    wave = sorted(range(n), key=lambda c: (c // 4 + (c % 4 + 1) // 2, c))

    def source_of(turn):
        code = sum(jnp.where(turn == spot, value, 0) for spot, value in enumerate(wave))
        k = code // 4
        rest = lax.rem(code, 4)
        edge = jnp.minimum(z, depth - 1 - z)
        near = z + jnp.where(lax.rem(k, 2) == 1, -((k + 1) // 2), k // 2)
        wide = jnp.where(2 * z < depth - 1, k, depth - 1 - k)
        s_z = jnp.where(k <= 2 * edge, near, wide)
        s_y = lax.rem(y + rest // 2, 2)
        s_x = lax.rem(x + lax.rem(rest, 2), 2)
        return s_z * 4 + s_y * 2 + s_x

    for stream in [streams] + list(range(streams)):
        each_copy(me, stream, True, lambda copy: copy.start())

    chunks = [slice(c, c + lanes) for c in range(0, width, lanes)]

    for g in range(groups):
        for h in range(GROUP):
            column = (g * GROUP + h) * HD
            att[h * rows:(h + 1) * rows, :] = q_ref[:, column:column + HD]
        q_t[g] = att[...].T

    lane = lax.rem(lax.broadcasted_iota(jnp.int32, (1, width), 1), rows)
    place_row[...] = jnp.where(lane < half, first_ref[0], first_ref[half])

    def attend_own(g):
        key_rows = k_ref[:, g * HD:(g + 1) * HD]
        value_rows = v_ref[:, g * HD:(g + 1) * HD].T
        for cols in chunks:
            scores = jnp.dot(key_rows, q_t[g, :, cols], preferred_element_type=jnp.float32)
            key_row = lax.broadcasted_iota(jnp.int32, (rows, lanes), 0)
            query_row = lax.rem(lax.broadcasted_iota(jnp.int32, (1, lanes), 1) + cols.start, rows)
            seen = key_row <= query_row
            peak = jnp.max(jnp.where(seen, scores, -FAR), axis=0, keepdims=True)
            weights = jnp.where(seen, jnp.exp2((scores - peak) * scale), 0.0)
            top[g, :, cols] = peak
            total[g, :, cols] = jnp.sum(weights, axis=0, keepdims=True)
            acc[g, :, cols] = jnp.dot(
                value_rows, weights.astype(jnp.bfloat16), preferred_element_type=jnp.float32
            )

    def attend(source, g):
        key_rows = kv[source, 2 * g]
        value_rows = kv[source, 2 * g + 1].T
        mark = marks[source]
        firsts = [
            jnp.broadcast_to(mark[:, b * half:b * half + 1], (1, lanes)) for b in range(2)
        ]
        def score(number):
            return jnp.dot(key_rows, q_t[g, :, chunks[number]], preferred_element_type=jnp.float32)

        coming = score(0)
        for number, cols in enumerate(chunks):
            scores = coming
            if number + 1 < len(chunks):
                coming = score(number + 1)
            place = place_row[:, cols]
            old = top[g, :, cols]
            peak = old
            seen, blocks = [], []
            for b in range(2):
                block = scores[b * half:(b + 1) * half]
                visible = firsts[b] <= place
                peak = jnp.maximum(
                    peak, jnp.where(visible, jnp.max(block, axis=0, keepdims=True), -FAR)
                )
                seen.append(visible)
                blocks.append(block)
            shift = peak * scale
            factor = jnp.exp2((old - peak) * scale)
            weights = jnp.concatenate(
                [
                    jnp.exp2(blocks[b] * scale - jnp.where(seen[b], shift, FAR))
                    for b in range(2)
                ],
                axis=0,
            )
            top[g, :, cols] = peak
            total[g, :, cols] = total[g, :, cols] * factor + jnp.sum(weights, axis=0, keepdims=True)
            acc[g, :, cols] = acc[g, :, cols] * factor + jnp.dot(
                value_rows, weights.astype(jnp.bfloat16), preferred_element_type=jnp.float32
            )

    first = source_of(1)
    arrive(first, streams)
    for g in range(groups):
        attend_own(g)
        arrive(first, 2 * g)
        arrive(first, 2 * g + 1)

    def turn_body(turn, carry):
        source = source_of(turn)
        ahead = source_of(turn + 1)
        arrive(ahead, streams)
        for g in range(groups):
            arrive(ahead, 2 * g)
            arrive(ahead, 2 * g + 1)
            attend(source, g)
        return carry

    lax.fori_loop(1, n - 1, turn_body, 0)
    last = source_of(n - 1)
    for g in range(groups):
        attend(last, g)

    load_w.wait()
    for g in range(groups):
        share = (acc[g] * (1.0 / total[g])).astype(jnp.bfloat16)
        att[...] = share.T
        for h in range(GROUP):
            column = (g * GROUP + h) * HD
            part[:, column:column + HD] = att[h * rows:(h + 1) * rows, :]

    out_cols = out_ref.shape[1]
    tile = sent.shape[-1]
    tiles = out_cols // tile

    def product(owner, number):
        begin = pl.multiple_of(owner * out_cols + number * tile, tile)
        return jnp.dot(part[...], w[:, pl.ds(begin, tile)], preferred_element_type=jnp.float32)

    def out_copy(step, number):
        return pltpu.make_async_remote_copy(
            src_ref=sent.at[step - 1, number], dst_ref=got.at[step - 1, number],
            send_sem=out_send.at[step - 1, number], recv_sem=out_recv.at[step - 1, number],
            device_id=(me, lax.rem(head + step, heads)), device_id_type=MESH,
        )

    for step in range(1, heads):
        owner = lax.rem(head + step, heads)

        def send_tile(number, carry, step=step, owner=owner):
            sent[step - 1, number] = product(owner, number).astype(jnp.bfloat16)
            out_copy(step, number).start()
            return carry

        lax.fori_loop(0, tiles, send_tile, 0)

    def own_tile(number, carry):
        value = product(head, number)
        for step in range(1, heads):
            out_copy(step, number).wait_recv()
            value = value + got[step - 1, number].astype(jnp.float32)
        out_ref[:, pl.ds(pl.multiple_of(number * tile, tile), tile)] = value.astype(out_ref.dtype)
        return carry

    lax.fori_loop(0, tiles, own_tile, 0)

    def finish(number, carry):
        for step in range(1, heads):
            out_copy(step, number).wait_send()
        return carry

    lax.fori_loop(0, tiles, finish, 0)

    for stream in range(streams + 1):
        each_copy(me, stream, True, lambda copy: copy.wait_send())

    def close(turn, carry):
        source = source_of(turn)
        for stream in range(streams + 1):
            each_copy(source, stream, False, lambda copy: copy.wait_send())
        return carry

    lax.fori_loop(1, n, close, 0)


def shards(n, heads, queries, key_states, value_states, positions, out_weight):
    rows = queries.shape[0]
    groups = key_states.shape[1] // HD
    streams = 2 * groups
    width = GROUP * rows
    out_cols = out_weight.shape[1] // heads
    tile = min(1024, out_cols)
    tiles = out_cols // tile
    vmem = pl.BlockSpec(memory_space=pltpu.VMEM)
    bf16, f32 = jnp.bfloat16, jnp.float32
    dma = pltpu.SemaphoreType.DMA
    return pl.pallas_call(
        functools.partial(kernel, n, heads, 768),
        out_shape=jax.ShapeDtypeStruct((rows, out_cols), bf16),
        in_specs=[vmem] * 3 + [pl.BlockSpec(memory_space=pltpu.SMEM), vmem] + [pl.BlockSpec(memory_space=pl.ANY)],
        out_specs=vmem,
        scratch_shapes=[
            pltpu.VMEM((n, streams, rows, HD), bf16),
            pltpu.VMEM((n, 1, rows), jnp.int32),
            pltpu.VMEM((1, width), jnp.int32),
            pltpu.VMEM((groups, HD, width), bf16),
            pltpu.VMEM((groups, HD, width), f32),
            pltpu.VMEM((groups, 1, width), f32),
            pltpu.VMEM((groups, 1, width), f32),
            pltpu.VMEM((width, HD), bf16),
            pltpu.VMEM(out_weight.shape, bf16),
            pltpu.VMEM((rows, out_weight.shape[0]), bf16),
            pltpu.VMEM((heads - 1, tiles, rows, tile), bf16),
            pltpu.VMEM((heads - 1, tiles, rows, tile), bf16),
            dma((n, streams, 4)),
            dma((n, streams)),
            dma((n, 4)),
            dma((n,)),
            dma,
            dma((heads - 1, tiles)),
            dma((heads - 1, tiles)),
        ],
        compiler_params=pltpu.CompilerParams(
            collective_id=0, has_side_effects=True, vmem_limit_bytes=60000 * 1024
        ),
    )(queries, key_states, value_states, positions, positions[None], out_weight)


def solution(mesh):
    in_specs = (P("seq", "head"), P("seq", "head"), P("seq", "head"), P("seq"), P("head", None))
    out_specs = P("seq", "head")
    body = functools.partial(shards, mesh.shape["seq"], mesh.shape["head"])
    return jax.shard_map(body, mesh=mesh, in_specs=in_specs, out_specs=out_specs, check_vma=False)
```
